32 devices in a mesh: sph: 8 (over z, core), rad: 4 (over y, x).
Axes of the slice: x: 2, y: 2, z: 4, core: 2. Of those that a mesh axis runs over, the one named last changes fastest.
Arguments:
- coeffs: bfloat16 [32768, 480], P('sph'), may hold values from -6 to 6
- interp: bfloat16 [32768, 2048], P('sph', 'rad'), may hold values from -0.06591797 to 0.06591797
- phases: float32 [64, 2048], P(None, 'rad'), may hold values from 0.3 to 3
- tables: bfloat16 [16, 480, 480], P('rad'), may hold values from -0.25 to 0.25
- bins: int32 [32768], P('sph'), may hold values from 0 to 63
Outputs:
- fields: bfloat16 [32768, 480], P('sph', 'rad')
The draws below stay inside these ranges and needn't reach their ends.
All inputs are finite; a program needn't handle non-finite values.
Results may differ from the reference program's by a relative error of at most 0.024.
Values may be sent and summed in bfloat16 or wider, within the bound.
A program may use at most 64 MiB of HBM per device.

```python
import math
import jax
import jax.numpy as jnp
from jax import lax

C = 240
C2 = 480
R = 2048
TBL = 128
NB = 16
NH = 64
S_DEV = 4096
S = 32768
N_SPH = 8


def with_ends(drawn, key, low, top_value):
    longest = drawn.shape.index(max(drawn.shape))
    spots = []
    for shift in (0, 1):
        where = [jax.random.randint(jax.random.fold_in(key, axis), (), 0, length) for axis, length in enumerate(drawn.shape)]
        where[longest] = (where[longest] + shift) % drawn.shape[longest]
        spots.append(tuple(where))
    return drawn.at[spots[0]].set(low).at[spots[1]].set(top_value)


def steps_of(own_key, dims, pieces, low, high):
    def one(axis_at, blocks):
        draws = jax.random.uniform(jax.random.fold_in(jax.random.fold_in(own_key, 6), axis_at), (blocks,), jnp.float32, low / len(pieces), high / len(pieces))
        return jnp.repeat(jnp.exp(draws), dims[axis_at] // blocks).reshape((-1,) + (1,) * (len(dims) - axis_at - 1))

    factor_of = one(*pieces[0])
    for cut in pieces[1:]:
        factor_of = factor_of * one(*cut)
    return factor_of


def noise(key, shape, deviation, reach, pieces=(), held_as=jnp.bfloat16):
    entries = deviation * jax.random.normal(key, shape, jnp.float32)
    if pieces:
        entries = entries * steps_of(key, shape, pieces, -0.22, 0.18)
    return jnp.clip(entries, -reach, reach).astype(held_as)


def setup_inputs(seed: int = 0) -> dict:
    arg_keys = jax.random.split(jax.random.key(seed), 6)
    return {
        "coeffs": noise(arg_keys[0], (S, C2), 1.0, 6.0, ((0, 8),)),
        "interp": noise(arg_keys[1], (S, R), ((S_DEV * N_SPH * R) ** -0.25), 0.06591797, ((0, 8), (1, 4))),
        "phases": jnp.clip(jnp.exp(math.log(3.0) - 2.3025851 * jax.random.uniform(arg_keys[2], (NH, R), jnp.float32) ** steps_of(arg_keys[2], (NH, R), ((1, 4),), -0.2, 0.2)), 0.3, 3.0),
        "tables": noise(arg_keys[3], (NB, C2, C2), (2 * C) ** -0.5, 0.25, ((0, 4),)),
        "bins": with_ends(jax.random.randint(arg_keys[4], (S,), 0, NH), jax.random.fold_in(arg_keys[4], 1), 0, NH - 1).astype(jnp.int32),
    }


def reference(coeffs, interp, phases, tables, bins):
    lifted = phases[bins]
    proj = (interp.astype(jnp.float32) * lifted).astype(jnp.bfloat16)
    nodes_sum = jnp.dot(proj.T, coeffs, preferred_element_type=jnp.float32)
    nodes = nodes_sum.astype(jnp.bfloat16)
    blocks = nodes.reshape(tables.shape[0], TBL, tables.shape[1]).astype(jnp.float32)
    angular = jnp.einsum("btc,bcd->btd", blocks, tables.astype(jnp.float32), precision=lax.Precision.HIGHEST)
    angular = angular.reshape(nodes.shape[0], nodes.shape[1]).astype(jnp.bfloat16)
    return jnp.dot(proj, angular, preferred_element_type=jnp.float32).astype(jnp.bfloat16)
```

```python
import functools

import jax
import jax.numpy as jnp
from jax import lax
from jax.experimental import pallas as pl
from jax.experimental.pallas import tpu as pltpu
from jax.sharding import PartitionSpec as P

MESH = pl.DeviceIdType.MESH
F32, BF16 = jnp.float32, jnp.bfloat16


def plain_body(coeffs, interp, phases, tables, bins):
    node_rows = interp.shape[1]
    onehot = (bins[:, None] == jnp.arange(phases.shape[0], dtype=jnp.int32)[None, :]).astype(F32)
    lifted = jnp.dot(onehot, phases, precision=lax.Precision.HIGHEST, preferred_element_type=F32)
    proj = (interp.astype(F32) * lifted).astype(BF16)
    partial_nodes = jnp.einsum("sr,sc->rc", proj, coeffs, preferred_element_type=F32)
    share = lax.psum_scatter(partial_nodes.astype(BF16), "sph", scatter_dimension=0, tiled=True)
    rows = share.shape[0]
    which = lax.axis_index("sph") * rows // (node_rows // tables.shape[0])
    table = lax.dynamic_index_in_dim(tables, which, 0, keepdims=False)
    local_part = jnp.dot(share, table, preferred_element_type=F32).astype(BF16)
    angular = lax.all_gather(local_part, "sph", axis=0, tiled=True)
    terms = jnp.dot(proj, angular, preferred_element_type=F32)
    return lax.psum_scatter(terms.astype(BF16), "rad", scatter_dimension=1, tiled=True)


def kernel(
    n_sph, n_chunks,
    coeffs_hbm, interp_hbm, phases_ref, tables_hbm, bins_ref, out_ref,
    coeffs, interp, table, lift_w, projt, acc,
    pair_out, pair_in, line_out, line_in, ang, angt,
    s1_out, s1_in, s2_out, s2_in, keep,
    load_sem, table_sem, pair_sem, line_sem, gather_sem, relay_sem, s1_sem, s2_sem,
):
    sph, rad = lax.axis_index("sph"), lax.axis_index("rad")
    n_z = n_sph // 2
    z, core = sph // 2, sph % 2
    y, x = rad // 2, rad % 2
    other_core = z * 2 + 1 - core
    across_x, across_y = y * 2 + 1 - x, (1 - y) * 2 + x
    chunk = projt.shape[2]
    nodes, cols = projt.shape[1], coeffs.shape[2]
    rows = acc.shape[1]
    block = cols // 4
    half = n_chunks // 2

    def along(d):
        return ((z + d) % n_z) * 2 + core

    def origin(d):
        return (z + n_z - d) % n_z

    def loads(k):
        at = pl.ds(k * chunk, chunk)
        return (
            pltpu.make_async_copy(interp_hbm.at[at], interp.at[k], load_sem.at[0, k]),
            pltpu.make_async_copy(coeffs_hbm.at[at], coeffs.at[k], load_sem.at[1, k]),
        )

    for k in range(n_chunks):
        for copy in loads(k):
            copy.start()
    which = sph * rows // (nodes // tables_hbm.shape[0])
    table_copy = pltpu.make_async_copy(tables_hbm.at[which], table, table_sem)
    table_copy.start()

    barrier = pltpu.get_barrier_semaphore()
    partners = [(other_core, rad)] + [(along(d), rad) for d in range(1, n_z)]
    partners += [(sph, across_x), (sph, across_y)]
    for partner in partners:
        pl.semaphore_signal(barrier, inc=1, device_id=partner, device_id_type=MESH)

    whole = phases_ref[...]
    hi = whole.astype(BF16).astype(F32)
    mid = (whole - hi).astype(BF16).astype(F32)
    lo = (whole - hi) - mid
    parts = jnp.concatenate([hi, mid, lo, jnp.zeros_like(hi)], axis=0)
    lift_w[...] = parts.T.astype(BF16)
    acc[...] = jnp.zeros_like(acc)

    def project(k, carry):
        a, b = loads(k)
        a.wait()
        here = bins_ref[k]
        level = lax.broadcasted_iota(jnp.int32, (whole.shape[0], chunk), 0)
        hot = jnp.where(level == here, 1.0, 0.0).astype(BF16)
        lifted = jnp.dot(lift_w[...], jnp.concatenate([hot] * 4, axis=0), preferred_element_type=F32)
        projt[k] = (interp[k].T.astype(F32) * lifted).astype(BF16)
        b.wait()
        acc[...] += jnp.dot(projt[k], coeffs[k], preferred_element_type=F32).reshape(acc.shape)
        return carry

    lax.fori_loop(0, n_chunks, project, 0)

    for i in range(n_z):
        pair_out[i] = acc[2 * i + 1 - core].astype(BF16)
    pl.semaphore_wait(barrier, len(partners))

    def remote(src, dst, sems, at, device):
        return pltpu.make_async_remote_copy(
            src_ref=src, dst_ref=dst, send_sem=sems.at[(0, *at)], recv_sem=sems.at[(1, *at)],
            device_id=device, device_id_type=MESH,
        )

    pair = remote(pair_out, pair_in, pair_sem, (), (other_core, rad))
    pair.start()
    pair.wait_recv()
    sends = [
        remote(line_out.at[d - 1], line_in.at[d - 1], line_sem, (d - 1,), (along(d), rad))
        for d in range(1, n_z)
    ]
    for d in range(n_z - 1, 0, -1):
        to = (z + d) % n_z
        line_out[d - 1] = (acc[2 * to + core] + pair_in[to].astype(F32)).astype(BF16)
        sends[d - 1].start()
    total = acc[sph] + pair_in[z].astype(F32)
    for d in range(1, n_z):
        sends[d - 1].wait_recv()
        total = total + line_in[d - 1].astype(F32)
    table_copy.wait()
    ang[sph] = jnp.dot(total.astype(BF16), table[...], preferred_element_type=F32).astype(BF16)

    gathers = [
        remote(ang.at[sph], ang.at[sph], gather_sem, (d - 1,), (along(d), rad)) for d in range(1, n_z)
    ]
    relays = []
    for d in range(n_z):
        piece = ang.at[origin(d) * 2 + core]
        relays.append(remote(piece, piece, relay_sem, (d,), (other_core, rad)))
    for d in range(n_z - 1, 0, -1):
        gathers[d - 1].start()
    relays[0].start()
    for d in range(1, n_z):
        gathers[d - 1].wait_recv()
        relays[d].start()
    for d in range(n_z):
        relays[d].wait_recv()

    turned = ang[...].reshape(nodes, cols).astype(F32).T
    q = [turned[i * block:(i + 1) * block] for i in range(4)]
    for h, g, first, second in ((0, 0, 0, 2), (0, 1, 1, 3), (1, 0, 0, 1), (1, 1, 2, 3)):
        angt[h, g] = jnp.concatenate([q[first], q[second]], axis=0).astype(BF16)

    side = (x, y)
    first_to, second_to = (across_x, across_y), (across_y, across_x)

    def stage1(h, k):
        return remote(s1_out.at[h, k], s1_in.at[h, k], s1_sem, (h, k), (sph, first_to[h]))

    def stage2(h, k):
        return remote(s2_out.at[h, k], s2_in.at[h, k], s2_sem, (h, k), (sph, second_to[h]))

    def give(k, carry):
        for h in range(2):
            s1_out[h, k] = jnp.dot(
                angt[h, 1 - side[h]], projt[h * half + k], preferred_element_type=F32
            ).astype(BF16)
            stage1(h, k).start()
        return carry

    lax.fori_loop(0, half, give, 0)

    def join(k, carry):
        for h in range(2):
            mine = jnp.dot(angt[h, side[h]], projt[h * half + k], preferred_element_type=F32)
            stage1(h, k).wait_recv()
            mine = mine + s1_in[h, k].astype(F32)
            low, high = mine[:block], mine[block:]
            lower = side[1 - h] == 0
            keep[h, k] = jnp.where(lower, low, high)
            away = jnp.where(lower, high, low)
            s2_out[h, k] = jnp.concatenate([away[:, :chunk // 2], away[:, chunk // 2:]], axis=0).astype(BF16)
            stage2(h, k).start()
        return carry

    lax.fori_loop(0, half, join, 0)

    def finish(k, carry):
        for h in range(2):
            stage2(h, k).wait_recv()
            got = s2_in[h, k].astype(F32)
            field = keep[h, k] + jnp.concatenate([got[:block], got[block:]], axis=1)
            out_ref[pl.ds(pl.multiple_of((h * half + k) * chunk, chunk), chunk)] = field.T.astype(BF16)
        return carry

    lax.fori_loop(0, half, finish, 0)

    pair.wait_send()
    for copy in sends + gathers + relays:
        copy.wait_send()

    def drain(k, carry):
        for h in range(2):
            stage1(h, k).wait_send()
            stage2(h, k).wait_send()
        return carry

    lax.fori_loop(0, half, drain, 0)


def fused_body(n_sph, n_rad, chunk, coeffs, interp, phases, tables, bins):
    spheres, nodes = interp.shape
    cols = coeffs.shape[1]
    n_chunks = spheres // chunk
    half, rows, n_z, block = n_chunks // 2, nodes // n_sph, n_sph // 2, cols // n_rad
    levels = phases.shape[0]
    vmem = pl.BlockSpec(memory_space=pltpu.VMEM)
    hbm = pl.BlockSpec(memory_space=pl.ANY)
    dma = pltpu.SemaphoreType.DMA
    return pl.pallas_call(
        functools.partial(kernel, n_sph, n_chunks),
        out_shape=jax.ShapeDtypeStruct((spheres, block), BF16),
        in_specs=[hbm, hbm, vmem, hbm, vmem],
        out_specs=vmem,
        scratch_shapes=[
            pltpu.VMEM((n_chunks, chunk, cols), BF16),
            pltpu.VMEM((n_chunks, chunk, nodes), BF16),
            pltpu.VMEM((cols, cols), BF16),
            pltpu.VMEM((nodes, 4 * levels), BF16),
            pltpu.VMEM((n_chunks, nodes, chunk), BF16),
            pltpu.VMEM((n_sph, rows, cols), F32),
            pltpu.VMEM((n_z, rows, cols), BF16),
            pltpu.VMEM((n_z, rows, cols), BF16),
            pltpu.VMEM((n_z - 1, rows, cols), BF16),
            pltpu.VMEM((n_z - 1, rows, cols), BF16),
            pltpu.VMEM((n_sph, rows, cols), BF16),
            pltpu.VMEM((2, 2, 2 * block, nodes), BF16),
            pltpu.VMEM((2, half, 2 * block, chunk), BF16),
            pltpu.VMEM((2, half, 2 * block, chunk), BF16),
            pltpu.VMEM((2, half, 2 * block, chunk // 2), BF16),
            pltpu.VMEM((2, half, 2 * block, chunk // 2), BF16),
            pltpu.VMEM((2, half, block, chunk), F32),
            dma((2, n_chunks)),
            dma,
            dma((2,)),
            dma((2, n_z - 1)),
            dma((2, n_z - 1)),
            dma((2, n_z)),
            dma((2, 2, half)),
            dma((2, 2, half)),
        ],
        compiler_params=pltpu.CompilerParams(
            collective_id=0, has_side_effects=True, vmem_limit_bytes=60 * 1024 * 1024
        ),
    )(coeffs, interp, phases, tables, bins.reshape(n_chunks, 1, chunk))


def solution(mesh):
    n_sph, n_rad = mesh.shape["sph"], mesh.shape["rad"]

    def body(coeffs, interp, phases, tables, bins):
        spheres, nodes = interp.shape
        chunk = spheres // 8
        fits = (
            n_rad == 4
            and n_sph % 2 == 0
            and n_sph >= 4
            and coeffs.shape[1] % (8 * n_rad) == 0
            and nodes % (16 * n_sph) == 0
            and (nodes // tables.shape[0]) % (nodes // n_sph) == 0
            and spheres % 8 == 0
            and chunk % 256 == 0
        )
        if fits:
            return fused_body(n_sph, n_rad, chunk, coeffs, interp, phases, tables, bins)
        return plain_body(coeffs, interp, phases, tables, bins)

    return jax.shard_map(
        body,
        mesh=mesh,
        in_specs=(P("sph", None), P("sph", "rad"), P(None, "rad"), P("rad", None, None), P("sph")),
        out_specs=P("sph", "rad"),
        check_vma=False,
    )
```

```python
import functools

import jax
import jax.numpy as jnp
from jax import lax
from jax.experimental import pallas as pl
from jax.experimental.pallas import tpu as pltpu
from jax.sharding import PartitionSpec as P

MESH = pl.DeviceIdType.MESH
F32, BF16 = jnp.float32, jnp.bfloat16


def plain_body(coeffs, interp, phases, tables, bins):
    node_rows = interp.shape[1]
    onehot = (bins[:, None] == jnp.arange(phases.shape[0], dtype=jnp.int32)[None, :]).astype(F32)
    lifted = jnp.dot(onehot, phases, precision=lax.Precision.HIGHEST, preferred_element_type=F32)
    proj = (interp.astype(F32) * lifted).astype(BF16)
    partial_nodes = jnp.einsum("sr,sc->rc", proj, coeffs, preferred_element_type=F32)
    share = lax.psum_scatter(partial_nodes.astype(BF16), "sph", scatter_dimension=0, tiled=True)
    rows = share.shape[0]
    which = lax.axis_index("sph") * rows // (node_rows // tables.shape[0])
    table = lax.dynamic_index_in_dim(tables, which, 0, keepdims=False)
    local_part = jnp.dot(share, table, preferred_element_type=F32).astype(BF16)
    angular = lax.all_gather(local_part, "sph", axis=0, tiled=True)
    terms = jnp.dot(proj, angular, preferred_element_type=F32)
    return lax.psum_scatter(terms.astype(BF16), "rad", scatter_dimension=1, tiled=True)


def kernel(
    n_sph, n_chunks,
    coeffs_hbm, interp_hbm, phases_ref, tables_hbm, bins_ref, out_ref,
    coeffs, interp, table, lift_w, projt, acc,
    pair_out, pair_in, line_out, line_in, ang, angt, sent, got,
    load_sem, table_sem, pair_sem, line_sem, gather_sem, relay_sem, field_sem,
):
    sph, rad = lax.axis_index("sph"), lax.axis_index("rad")
    n_z = n_sph // 2
    z, core = sph // 2, sph % 2
    y, x = rad // 2, rad % 2
    other_core = z * 2 + 1 - core
    across_x, across_y = y * 2 + 1 - x, (1 - y) * 2 + x
    chunk = projt.shape[2]
    nodes, cols = projt.shape[1], coeffs.shape[1]
    rows = acc.shape[1]
    block = cols // 4
    half = n_chunks // 2

    def along(d):
        return ((z + d) % n_z) * 2 + core

    def origin(d):
        return (z + n_z - d) % n_z

    def loads(k):
        at = pl.ds(k * chunk, chunk)
        return (
            pltpu.make_async_copy(interp_hbm.at[at], interp.at[k], load_sem.at[0, k]),
            pltpu.make_async_copy(coeffs_hbm.at[:, at], coeffs.at[k], load_sem.at[1, k]),
        )

    for k in range(n_chunks):
        for copy in loads(k):
            copy.start()
    which = sph * rows // (nodes // tables_hbm.shape[0])
    table_copy = pltpu.make_async_copy(tables_hbm.at[which], table, table_sem)
    table_copy.start()

    barrier = pltpu.get_barrier_semaphore()
    partners = [(other_core, rad)] + [(along(d), rad) for d in range(1, n_z)]
    partners += [(sph, across_x), (sph, across_y)]
    for partner in partners:
        pl.semaphore_signal(barrier, inc=1, device_id=partner, device_id_type=MESH)

    whole = phases_ref[...]
    hi = whole.astype(BF16).astype(F32)
    mid = (whole - hi).astype(BF16).astype(F32)
    lo = (whole - hi) - mid
    parts = jnp.concatenate([hi, mid, lo, jnp.zeros_like(hi)], axis=0)
    lift_w[...] = parts.T.astype(BF16)
    acc[...] = jnp.zeros_like(acc)

    def project(k, carry):
        a, b = loads(k)
        a.wait()
        here = bins_ref[k]
        level = lax.broadcasted_iota(jnp.int32, (whole.shape[0], chunk), 0)
        hot = jnp.where(level == here, 1.0, 0.0).astype(BF16)
        lifted = jnp.dot(lift_w[...], jnp.concatenate([hot] * 4, axis=0), preferred_element_type=F32)
        projt[k] = (interp[k].T.astype(F32) * lifted).astype(BF16)
        b.wait()
        acc[...] += lax.dot_general(
            projt[k], coeffs[k], (((1,), (1,)), ((), ())), preferred_element_type=F32
        ).reshape(acc.shape)
        return carry

    lax.fori_loop(0, n_chunks, project, 0)

    for i in range(n_z):
        pair_out[i] = acc[2 * i + 1 - core].astype(BF16)
    pl.semaphore_wait(barrier, len(partners))

    def remote(src, dst, sems, at, device):
        return pltpu.make_async_remote_copy(
            src_ref=src, dst_ref=dst, send_sem=sems.at[(0, *at)], recv_sem=sems.at[(1, *at)],
            device_id=device, device_id_type=MESH,
        )

    def gather(p, d):
        mine = ang.at[p, sph, pl.ds(0, 1 + 2 * p)]
        return remote(mine, mine, gather_sem, (p, d - 1), (along(d), rad))

    def relay(p, d):
        piece = ang.at[p, origin(d) * 2 + core, pl.ds(0, 1 + 2 * p)]
        return remote(piece, piece, relay_sem, (p, d), (other_core, rad))

    pair = remote(pair_out, pair_in, pair_sem, (), (other_core, rad))
    pair.start()
    pair.wait_recv()
    sends = [
        remote(line_out.at[d - 1], line_in.at[d - 1], line_sem, (d - 1,), (along(d), rad))
        for d in range(1, n_z)
    ]
    for d in range(n_z - 1, 0, -1):
        to = (z + d) % n_z
        line_out[d - 1] = (acc[2 * to + core] + pair_in[to].astype(F32)).astype(BF16)
        sends[d - 1].start()
    total = acc[sph] + pair_in[z].astype(F32)
    for d in range(1, n_z):
        sends[d - 1].wait_recv()
        total = total + line_in[d - 1].astype(F32)
    table_copy.wait()
    share = jnp.dot(total.astype(BF16), table[...], preferred_element_type=F32)
    q = [share[:, i * block:(i + 1) * block] for i in range(4)]
    far_row = [jnp.where(y == 0, q[2 + i], q[i]) for i in range(2)]
    near_row = [jnp.where(y == 0, q[i], q[2 + i]) for i in range(2)]
    diagonal = jnp.where(x == 0, far_row[1], far_row[0])
    same_x = jnp.where(x == 0, far_row[0], far_row[1])
    same_y = jnp.where(x == 0, near_row[1], near_row[0])
    own = jnp.where(x == 0, near_row[0], near_row[1])
    for i, part in enumerate((diagonal, same_x, same_y, own)):
        ang[min(i, 1), sph, max(i - 1, 0)] = part.astype(BF16)
        if i == 0 or i == 3:
            p = min(i, 1)
            for d in range(n_z - 1, 0, -1):
                gather(p, d).start()
            relay(p, 0).start()

    def collect(p):
        for d in range(1, n_z):
            gather(p, d).wait_recv()
            relay(p, d).start()
        for d in range(n_z):
            relay(p, d).wait_recv()

    first_to, second_to = (across_x, across_y), (across_y, across_x)

    def field(stage, h, k):
        to = second_to[h] if stage == 1 else first_to[h]
        return remote(sent.at[stage, h, k], got.at[stage, h, k], field_sem, (stage, h, k), (sph, to))

    def terms(i, h, k):
        return jnp.dot(angt[i], projt[h * half + k], preferred_element_type=F32)

    def pack(v):
        return jnp.concatenate([v[:, :chunk // 2], v[:, chunk // 2:]], axis=0).astype(BF16)

    def unpack(v):
        v = v.astype(F32)
        return jnp.concatenate([v[:block], v[block:]], axis=1)

    collect(0)
    angt[0] = ang[0, :, 0].reshape(nodes, block).astype(F32).T.astype(BF16)

    def give(k, carry):
        for h in range(2):
            sent[0, h, k] = pack(terms(0, h, k))
            field(0, h, k).start()
        return carry

    lax.fori_loop(0, half, give, 0)

    collect(1)
    for i in range(3):
        angt[1 + i] = ang[1, :, i].reshape(nodes, block).astype(F32).T.astype(BF16)

    def join(k, carry):
        for h in range(2):
            sent[2, h, k] = pack(terms(2 - h, h, k))
            mine = terms(1 + h, h, k)
            field(0, h, k).wait_recv()
            sent[1, h, k] = pack(mine + unpack(got[0, h, k]))
            field(1, h, k).start()
            field(2, h, k).start()
        return carry

    lax.fori_loop(0, half, join, 0)

    def finish(k, carry):
        for h in range(2):
            mine = terms(3, h, k)
            field(1, h, k).wait_recv()
            field(2, h, k).wait_recv()
            mine = mine + unpack(got[1, h, k]) + unpack(got[2, h, k])
            out_ref[:, pl.ds(pl.multiple_of((h * half + k) * chunk, chunk), chunk)] = mine.astype(BF16)
        return carry

    lax.fori_loop(0, half, finish, 0)

    pair.wait_send()
    for copy in sends:
        copy.wait_send()
    for p in range(2):
        for d in range(1, n_z):
            gather(p, d).wait_send()
        for d in range(n_z):
            relay(p, d).wait_send()

    def drain(k, carry):
        for h in range(2):
            for stage in range(3):
                field(stage, h, k).wait_send()
        return carry

    lax.fori_loop(0, half, drain, 0)


def fused_body(n_sph, n_rad, chunk, coeffs, interp, phases, tables, bins):
    spheres, nodes = interp.shape
    cols = coeffs.shape[1]
    n_chunks = spheres // chunk
    half, rows, n_z, block = n_chunks // 2, nodes // n_sph, n_sph // 2, cols // n_rad
    levels = phases.shape[0]
    vmem = pl.BlockSpec(memory_space=pltpu.VMEM)
    hbm = pl.BlockSpec(memory_space=pl.ANY)
    dma = pltpu.SemaphoreType.DMA
    return pl.pallas_call(
        functools.partial(kernel, n_sph, n_chunks),
        out_shape=jax.ShapeDtypeStruct((block, spheres), BF16),
        in_specs=[hbm, hbm, vmem, hbm, vmem],
        out_specs=vmem,
        scratch_shapes=[
            pltpu.VMEM((n_chunks, cols, chunk), BF16),
            pltpu.VMEM((n_chunks, chunk, nodes), BF16),
            pltpu.VMEM((cols, cols), BF16),
            pltpu.VMEM((nodes, 4 * levels), BF16),
            pltpu.VMEM((n_chunks, nodes, chunk), BF16),
            pltpu.VMEM((n_sph, rows, cols), F32),
            pltpu.VMEM((n_z, rows, cols), BF16),
            pltpu.VMEM((n_z, rows, cols), BF16),
            pltpu.VMEM((n_z - 1, rows, cols), BF16),
            pltpu.VMEM((n_z - 1, rows, cols), BF16),
            pltpu.VMEM((2, n_sph, 3, rows, block), BF16),
            pltpu.VMEM((4, block, nodes), BF16),
            pltpu.VMEM((3, 2, half, 2 * block, chunk // 2), BF16),
            pltpu.VMEM((3, 2, half, 2 * block, chunk // 2), BF16),
            dma((2, n_chunks)),
            dma,
            dma((2,)),
            dma((2, n_z - 1)),
            dma((2, 2, n_z - 1)),
            dma((2, 2, n_z)),
            dma((2, 3, 2, half)),
        ],
        compiler_params=pltpu.CompilerParams(
            collective_id=0, has_side_effects=True, vmem_limit_bytes=60 * 1024 * 1024
        ),
    )(coeffs.T, interp, phases, tables, bins.reshape(n_chunks, 1, chunk)).T


def solution(mesh):
    n_sph, n_rad = mesh.shape["sph"], mesh.shape["rad"]

    def body(coeffs, interp, phases, tables, bins):
        spheres, nodes = interp.shape
        chunk = spheres // 8
        fits = (
            n_rad == 4
            and n_sph % 2 == 0
            and n_sph >= 4
            and coeffs.shape[1] % (8 * n_rad) == 0
            and nodes % (16 * n_sph) == 0
            and (nodes // tables.shape[0]) % (nodes // n_sph) == 0
            and spheres % 8 == 0
            and chunk % 256 == 0
        )
        if fits:
            return fused_body(n_sph, n_rad, chunk, coeffs, interp, phases, tables, bins)
        return plain_body(coeffs, interp, phases, tables, bins)

    return jax.shard_map(
        body,
        mesh=mesh,
        in_specs=(P("sph", None), P("sph", "rad"), P(None, "rad"), P("rad", None, None), P("sph")),
        out_specs=P("sph", "rad"),
        check_vma=False,
    )
```

```python
import functools

import jax
import jax.numpy as jnp
from jax import lax
from jax.experimental import pallas as pl
from jax.experimental.pallas import tpu as pltpu
from jax.sharding import PartitionSpec as P

MESH = pl.DeviceIdType.MESH
F32, BF16 = jnp.float32, jnp.bfloat16


def plain_body(coeffs, interp, phases, tables, bins):
    node_rows = interp.shape[1]
    onehot = (bins[:, None] == jnp.arange(phases.shape[0], dtype=jnp.int32)[None, :]).astype(F32)
    lifted = jnp.dot(onehot, phases, precision=lax.Precision.HIGHEST, preferred_element_type=F32)
    proj = (interp.astype(F32) * lifted).astype(BF16)
    partial_nodes = jnp.einsum("sr,sc->rc", proj, coeffs, preferred_element_type=F32)
    share = lax.psum_scatter(partial_nodes.astype(BF16), "sph", scatter_dimension=0, tiled=True)
    rows = share.shape[0]
    which = lax.axis_index("sph") * rows // (node_rows // tables.shape[0])
    table = lax.dynamic_index_in_dim(tables, which, 0, keepdims=False)
    local_part = jnp.dot(share, table, preferred_element_type=F32).astype(BF16)
    angular = lax.all_gather(local_part, "sph", axis=0, tiled=True)
    terms = jnp.dot(proj, angular, preferred_element_type=F32)
    return lax.psum_scatter(terms.astype(BF16), "rad", scatter_dimension=1, tiled=True)


def kernel(
    n_sph, n_chunks,
    coeffs_hbm, interp_hbm, phases_ref, tables_hbm, bins_ref, out_ref,
    coeffs, interp, table, lift_w, projt, acc,
    pair_out, pair_in, line_out, line_in, ang, angt, sent, got,
    load_sem, table_sem, pair_sem, line_sem, gather_sem, relay_sem, field_sem,
):
    sph, rad = lax.axis_index("sph"), lax.axis_index("rad")
    n_z = n_sph // 2
    z, core = sph // 2, sph % 2
    y, x = rad // 2, rad % 2
    other_core = z * 2 + 1 - core
    across_x, across_y = y * 2 + 1 - x, (1 - y) * 2 + x
    chunk = projt.shape[2]
    nodes, cols = projt.shape[1], coeffs.shape[1]
    rows = acc.shape[1]
    block = cols // 4
    half = n_chunks // 2

    def along(d):
        return ((z + d) % n_z) * 2 + core

    def origin(d):
        return (z + n_z - d) % n_z

    def loads(k):
        at = pl.ds(k * chunk, chunk)
        return (
            pltpu.make_async_copy(interp_hbm.at[at], interp.at[k], load_sem.at[0, k]),
            pltpu.make_async_copy(coeffs_hbm.at[:, at], coeffs.at[k], load_sem.at[1, k]),
        )

    for k in range(n_chunks):
        for copy in loads(k):
            copy.start()
    which = sph * rows // (nodes // tables_hbm.shape[0])
    table_copy = pltpu.make_async_copy(tables_hbm.at[which], table, table_sem)
    table_copy.start()

    barrier = pltpu.get_barrier_semaphore()
    partners = [(other_core, rad)] + [(along(d), rad) for d in range(1, n_z)]
    partners += [(sph, across_x), (sph, across_y)]
    for partner in partners:
        pl.semaphore_signal(barrier, inc=1, device_id=partner, device_id_type=MESH)

    whole = phases_ref[...]
    hi = whole.astype(BF16).astype(F32)
    mid = (whole - hi).astype(BF16).astype(F32)
    lo = (whole - hi) - mid
    parts = jnp.concatenate([hi, mid, lo, jnp.zeros_like(hi)], axis=0)
    lift_w[...] = parts.T.astype(BF16)
    acc[...] = jnp.zeros_like(acc)

    def project(k, carry):
        a, b = loads(k)
        a.wait()
        here = bins_ref[k]
        level = lax.broadcasted_iota(jnp.int32, (whole.shape[0], chunk), 0)
        hot = jnp.where(level == here, 1.0, 0.0).astype(BF16)
        lifted = jnp.dot(lift_w[...], jnp.concatenate([hot] * 4, axis=0), preferred_element_type=F32)
        projt[k] = (interp[k].T.astype(F32) * lifted).astype(BF16)
        b.wait()
        acc[...] += lax.dot_general(
            projt[k], coeffs[k], (((1,), (1,)), ((), ())), preferred_element_type=F32
        ).reshape(acc.shape)
        return carry

    lax.fori_loop(0, n_chunks, project, 0)

    pl.semaphore_wait(barrier, len(partners))

    def remote(src, dst, sems, at, device):
        return pltpu.make_async_remote_copy(
            src_ref=src, dst_ref=dst, send_sem=sems.at[(0, *at)], recv_sem=sems.at[(1, *at)],
            device_id=device, device_id_type=MESH,
        )

    def gather(p, d):
        mine = ang.at[p, sph, pl.ds(0, 1 + 2 * p)]
        return remote(mine, mine, gather_sem, (p, d - 1), (along(d), rad))

    def relay(p, d):
        piece = ang.at[p, origin(d) * 2 + core, pl.ds(0, 1 + 2 * p)]
        return remote(piece, piece, relay_sem, (p, d), (other_core, rad))

    pairs = [
        remote(pair_out.at[d], pair_in.at[d], pair_sem, (d,), (other_core, rad)) for d in range(n_z)
    ]
    for d in range(n_z - 1, -1, -1):
        pair_out[d] = acc[2 * ((z + d) % n_z) + 1 - core].astype(BF16)
        pairs[d].start()
    sends = [
        remote(line_out.at[d - 1], line_in.at[d - 1], line_sem, (d - 1,), (along(d), rad))
        for d in range(1, n_z)
    ]
    for d in range(n_z - 1, 0, -1):
        to = (z + d) % n_z
        pairs[d].wait_recv()
        line_out[d - 1] = (acc[2 * to + core] + pair_in[d].astype(F32)).astype(BF16)
        sends[d - 1].start()
    pairs[0].wait_recv()
    total = acc[sph] + pair_in[0].astype(F32)
    for d in range(1, n_z):
        sends[d - 1].wait_recv()
        total = total + line_in[d - 1].astype(F32)
    table_copy.wait()
    share = jnp.dot(total.astype(BF16), table[...], preferred_element_type=F32)
    q = [share[:, i * block:(i + 1) * block] for i in range(4)]
    far_row = [jnp.where(y == 0, q[2 + i], q[i]) for i in range(2)]
    near_row = [jnp.where(y == 0, q[i], q[2 + i]) for i in range(2)]
    diagonal = jnp.where(x == 0, far_row[1], far_row[0])
    same_x = jnp.where(x == 0, far_row[0], far_row[1])
    same_y = jnp.where(x == 0, near_row[1], near_row[0])
    own = jnp.where(x == 0, near_row[0], near_row[1])
    for i, part in enumerate((diagonal, same_x, same_y, own)):
        ang[min(i, 1), sph, max(i - 1, 0)] = part.astype(BF16)
        if i == 0 or i == 3:
            p = min(i, 1)
            for d in range(n_z - 1, 0, -1):
                gather(p, d).start()
            relay(p, 0).start()

    def collect(p):
        for d in range(1, n_z):
            gather(p, d).wait_recv()
            relay(p, d).start()
        for d in range(n_z):
            relay(p, d).wait_recv()

    first_to, second_to = (across_x, across_y), (across_y, across_x)

    def field(stage, h, k):
        to = second_to[h] if stage == 1 else first_to[h]
        return remote(sent.at[stage, h, k], got.at[stage, h, k], field_sem, (stage, h, k), (sph, to))

    def terms(i, h, k):
        return jnp.dot(angt[i], projt[h * half + k], preferred_element_type=F32)

    def pack(v):
        return jnp.concatenate([v[:, :chunk // 2], v[:, chunk // 2:]], axis=0).astype(BF16)

    def unpack(v):
        v = v.astype(F32)
        return jnp.concatenate([v[:block], v[block:]], axis=1)

    collect(0)
    angt[0] = ang[0, :, 0].reshape(nodes, block).astype(F32).T.astype(BF16)

    def give(k, carry):
        for h in range(2):
            sent[0, h, k] = pack(terms(0, h, k))
            field(0, h, k).start()
        return carry

    lax.fori_loop(0, half, give, 0)

    collect(1)
    for i in range(3):
        angt[1 + i] = ang[1, :, i].reshape(nodes, block).astype(F32).T.astype(BF16)

    def join(k, carry):
        for h in range(2):
            sent[2, h, k] = pack(terms(2 - h, h, k))
            mine = terms(1 + h, h, k)
            field(0, h, k).wait_recv()
            sent[1, h, k] = pack(mine + unpack(got[0, h, k]))
            field(1, h, k).start()
            field(2, h, k).start()
        return carry

    lax.fori_loop(0, half, join, 0)

    def finish(k, carry):
        for h in range(2):
            mine = terms(3, h, k)
            field(1, h, k).wait_recv()
            field(2, h, k).wait_recv()
            mine = mine + unpack(got[1, h, k]) + unpack(got[2, h, k])
            out_ref[:, pl.ds(pl.multiple_of((h * half + k) * chunk, chunk), chunk)] = mine.astype(BF16)
        return carry

    lax.fori_loop(0, half, finish, 0)

    for copy in pairs + sends:
        copy.wait_send()
    for p in range(2):
        for d in range(1, n_z):
            gather(p, d).wait_send()
        for d in range(n_z):
            relay(p, d).wait_send()

    def drain(k, carry):
        for h in range(2):
            for stage in range(3):
                field(stage, h, k).wait_send()
        return carry

    lax.fori_loop(0, half, drain, 0)


def fused_body(n_sph, n_rad, chunk, coeffs, interp, phases, tables, bins):
    spheres, nodes = interp.shape
    cols = coeffs.shape[1]
    n_chunks = spheres // chunk
    half, rows, n_z, block = n_chunks // 2, nodes // n_sph, n_sph // 2, cols // n_rad
    levels = phases.shape[0]
    vmem = pl.BlockSpec(memory_space=pltpu.VMEM)
    hbm = pl.BlockSpec(memory_space=pl.ANY)
    dma = pltpu.SemaphoreType.DMA
    return pl.pallas_call(
        functools.partial(kernel, n_sph, n_chunks),
        out_shape=pltpu.VMEM((block, spheres), BF16),
        in_specs=[hbm, hbm, vmem, hbm, vmem],
        out_specs=vmem,
        scratch_shapes=[
            pltpu.VMEM((n_chunks, cols, chunk), BF16),
            pltpu.VMEM((n_chunks, chunk, nodes), BF16),
            pltpu.VMEM((cols, cols), BF16),
            pltpu.VMEM((nodes, 4 * levels), BF16),
            pltpu.VMEM((n_chunks, nodes, chunk), BF16),
            pltpu.VMEM((n_sph, rows, cols), F32),
            pltpu.VMEM((n_z, rows, cols), BF16),
            pltpu.VMEM((n_z, rows, cols), BF16),
            pltpu.VMEM((n_z - 1, rows, cols), BF16),
            pltpu.VMEM((n_z - 1, rows, cols), BF16),
            pltpu.VMEM((2, n_sph, 3, rows, block), BF16),
            pltpu.VMEM((4, block, nodes), BF16),
            pltpu.VMEM((3, 2, half, 2 * block, chunk // 2), BF16),
            pltpu.VMEM((3, 2, half, 2 * block, chunk // 2), BF16),
            dma((2, n_chunks)),
            dma,
            dma((2, n_z)),
            dma((2, n_z - 1)),
            dma((2, 2, n_z - 1)),
            dma((2, 2, n_z)),
            dma((2, 3, 2, half)),
        ],
        compiler_params=pltpu.CompilerParams(
            collective_id=0, has_side_effects=True, vmem_limit_bytes=60 * 1024 * 1024
        ),
    )(coeffs.T, interp, phases, tables, bins.reshape(n_chunks, 1, chunk)).T


def solution(mesh):
    n_sph, n_rad = mesh.shape["sph"], mesh.shape["rad"]

    def body(coeffs, interp, phases, tables, bins):
        spheres, nodes = interp.shape
        chunk = spheres // 8
        fits = (
            n_rad == 4
            and n_sph % 2 == 0
            and n_sph >= 4
            and coeffs.shape[1] % (8 * n_rad) == 0
            and nodes % (16 * n_sph) == 0
            and (nodes // tables.shape[0]) % (nodes // n_sph) == 0
            and spheres % 8 == 0
            and chunk % 256 == 0
        )
        if fits:
            return fused_body(n_sph, n_rad, chunk, coeffs, interp, phases, tables, bins)
        return plain_body(coeffs, interp, phases, tables, bins)

    return jax.shard_map(
        body,
        mesh=mesh,
        in_specs=(P("sph", None), P("sph", "rad"), P(None, "rad"), P("rad", None, None), P("sph")),
        out_specs=P("sph", "rad"),
        check_vma=False,
    )
```
